32 devices in a mesh: pa: 32 (over z, y, x, core).
Axes of the slice: x: 2, y: 2, z: 4, core: 2. Of those that a mesh axis runs over, the one named last changes fastest.
Arguments:
- signal_real: float32 [4194304], P('pa'), may hold values from -6 to 6
- signal_imag: float32 [4194304], P('pa'), may hold values from -6 to 6
Outputs:
- spectrum_real: float32 [4194304], P('pa')
- spectrum_imag: float32 [4194304], P('pa')
The draws below stay inside these ranges and needn't reach their ends.
All inputs are finite; a program needn't handle non-finite values.
Results may differ from the reference program's by a relative error of at most 0.0003.
Values sent between devices are 32-bit elements.
A program may use at most 128 MiB of HBM per device.

```python
import jax
import jax.numpy as jnp

LENGTH = 4194304


def levels(own_key, extent, shards, low, largest):
    level, own = 1.0, jax.random.fold_in(own_key, 6)
    for dim, blocks in shards:
        draws = jnp.exp(jax.random.uniform(jax.random.fold_in(own, dim), (blocks,), jnp.float32, low / len(shards), largest / len(shards)))
        level = level * jnp.repeat(draws, extent[dim] // blocks).reshape([-1 if axis == dim else 1 for axis in range(len(extent))])
    return level


def noise(own_key, extent, width, most, cuts=(), kind=jnp.bfloat16):
    level = levels(own_key, extent, cuts, -0.22, 0.18) if cuts else 1.0
    drawn = jax.random.normal(own_key, extent, jnp.float32) * width * level
    return jnp.minimum(jnp.maximum(drawn, -most), most).astype(kind)


def setup_inputs(seed: int = 0) -> dict:
    splits = jax.random.split(jax.random.key(seed), 3)
    return {
        "signal_real": noise(splits[0], (LENGTH,), 1.0, 6.0, ((0, 32),), jnp.float32),
        "signal_imag": noise(splits[1], (LENGTH,), 1.0, 6.0, ((0, 32),), jnp.float32),
    }


def reference(signal_real, signal_imag):
    spectrum = jnp.fft.fft(signal_real + 1j * signal_imag, norm="ortho")
    return jnp.real(spectrum).astype(jnp.float32), jnp.imag(spectrum).astype(jnp.float32)
```

```python
import functools
import math

import jax
import jax.numpy as jnp
import numpy as np
from jax import lax
from jax.experimental import pallas as pl
from jax.experimental.pallas import tpu as pltpu
from jax.sharding import PartitionSpec as P

LANES = 128
MESH = pl.DeviceIdType.MESH


def phase(index, length):
    angles = (np.asarray(index, np.int64) % length) * (-2.0 * np.pi / length)
    return np.exp(1j * angles)


def split(table):
    high = table.astype(np.float32).astype(jnp.bfloat16)
    low = (table - high.astype(np.float64)).astype(np.float32).astype(jnp.bfloat16)
    return high, low


def left_table(matrix):
    real = np.concatenate(
        [
            np.concatenate([matrix.real, -matrix.imag], -1),
            np.concatenate([matrix.imag, matrix.real], -1),
        ],
        -2,
    )
    high, low = split(real)
    return np.concatenate([high, high, low], -1)


def right_table(matrix):
    real = np.concatenate(
        [
            np.concatenate([matrix.real, matrix.imag], -1),
            np.concatenate([-matrix.imag, matrix.real], -1),
        ],
        -2,
    )
    high, low = split(real)
    return np.concatenate([high, high, low], -2)


def parts(value, axis):
    high = value.astype(jnp.bfloat16)
    low = (value - high.astype(jnp.float32)).astype(jnp.bfloat16)
    return jnp.concatenate([high, low, high], axis)


def kernel(
    n, rows, s1, t1, t2, tw, t3, tw3, t4, out_re, out_im, b, y, s2, c2, r3, send_sem, recv_sem
):
    me = lax.axis_index("pa")
    block = 2 * rows
    ratio = n // rows

    def piece(ref, index):
        return ref.at[pl.ds(pl.multiple_of(index * block, block), block), :]

    def copy(src, dst, step, peer, owner, stage):
        return pltpu.make_async_remote_copy(
            src_ref=piece(src, peer),
            dst_ref=piece(dst, owner),
            send_sem=send_sem.at[peer],
            recv_sem=recv_sem.at[stage, owner],
            device_id=(peer,),
            device_id_type=MESH,
        )

    def send(src, dst, stage):
        def go(step, carry):
            peer = lax.rem(me + step, n)
            copy(src, dst, step, peer, me, stage).start()
            return carry

        lax.fori_loop(1, n, go, 0)
        piece(dst, me)[...] = piece(src, me)[...]

    def wait(src, dst, stage):
        def go(step, carry):
            peer = lax.rem(me + step, n)
            handle = copy(src, dst, step, peer, peer, stage)
            handle.wait_send()
            handle.wait_recv()
            return carry

        lax.fori_loop(1, n, go, 0)

    def dot(left, right):
        return jnp.dot(left, right, preferred_element_type=jnp.float32)

    send(s1, b, 0)
    wait(s1, b, 0)

    def first(r, carry):
        both = jnp.concatenate(
            [b[pl.ds(r, n, stride=block), :], b[pl.ds(r + rows, n, stride=block), :]], 0
        )
        got = dot(t1[r], parts(both, 0))
        y[pl.ds(r, n, stride=block), :] = got[:n]
        y[pl.ds(r + rows, n, stride=block), :] = got[n:]
        return carry

    lax.fori_loop(0, rows, first, 0, unroll=4)

    def second(a, carry):
        got = dot(t2[...], parts(piece(y, a)[...], 0))
        re, im = got[:rows], got[rows:]
        cs = piece(tw, a)[...]
        cos, sin = cs[:rows], cs[rows:]
        at = a // rows * block + lax.rem(a, rows)
        s2[pl.ds(at, rows, stride=2 * n), :] = re * cos - im * sin
        s2[pl.ds(at + rows, rows, stride=2 * n), :] = re * sin + im * cos
        return carry

    lax.fori_loop(0, n, second, 0, unroll=4)

    send(s2, c2, 1)
    wait(s2, c2, 1)

    def third(v, carry):
        both = piece(c2, v)[...]
        both = jnp.concatenate([both[:rows], both[rows:]], 1)
        got = dot(parts(both, 1), t3[...])
        re, im = got[:, :LANES], got[:, LANES:]
        cos, sin = tw3[0, pl.ds(v, 1), :], tw3[1, pl.ds(v, 1), :]
        y[pl.ds(pl.multiple_of(v * block, block), rows), :] = re * cos - im * sin
        y[pl.ds(pl.multiple_of(v * block + rows, rows), rows), :] = re * sin + im * cos
        return carry

    lax.fori_loop(0, n, third, 0, unroll=4)

    def fourth(j, carry):
        both = jnp.concatenate(
            [y[pl.ds(j, n, stride=block), :], y[pl.ds(j + rows, n, stride=block), :]], 0
        )
        got = dot(t4[...], parts(both, 0))
        b[pl.ds(j, n, stride=block), :] = got[:n]
        b[pl.ds(j + rows, n, stride=block), :] = got[n:]
        return carry

    lax.fori_loop(0, rows, fourth, 0, unroll=4)

    send(b, r3, 2)
    wait(b, r3, 2)

    group = LANES // rows
    tiles = n // group
    for tile in range(tiles):
        for half, out in enumerate((out_re, out_im)):
            square = jnp.concatenate(
                [
                    r3[pl.ds((tile * group + g) * block + half * rows, rows), :]
                    for g in range(group)
                ],
                0,
            )
            out[pl.ds(tile, LANES, stride=tiles), :] = square.T


def body(signal_real, signal_imag):
    n = lax.axis_size("pa")
    local_len = signal_real.shape[0]
    full_len = local_len * n
    second_len = LANES * n
    rows = local_len // second_len
    first_len = rows * n
    me = lax.axis_index("pa")

    ids = np.arange
    a, p, r = ids(n), ids(n), ids(rows)
    t1 = left_table(
        phase(a[None, :, None] * (p[None, None, :] * rows + r[:, None, None]), first_len)
    )
    t2 = left_table(phase(r[:, None] * r[None, :], rows))
    u = ids(LANES)
    t3 = right_table(phase(u[:, None] * u[None, :], LANES))
    tw3 = phase(a[:, None] * u[None, :], second_len)
    tw3 = np.stack([tw3.real, tw3.imag]).astype(np.float32)
    t4 = left_table(phase(a[:, None] * p[None, :], n) / math.sqrt(full_len))

    k1 = a[:, None] + n * r[None, :]
    fixed = phase(k1[:, :, None] * u[None, None, :], local_len)
    turn = phase(p[:, None, None] * k1[None, :, :], full_len)
    f_re, f_im = fixed.real.astype(np.float32), fixed.imag.astype(np.float32)
    m_re = jnp.asarray(turn.real.astype(np.float32))[me][:, :, None]
    m_im = jnp.asarray(turn.imag.astype(np.float32))[me][:, :, None]
    tw = jnp.stack([f_re * m_re - f_im * m_im, f_re * m_im + f_im * m_re], 1)
    tw = tw.reshape(2 * first_len, LANES)

    s1 = jnp.stack([signal_real.reshape(rows, LANES, n), signal_imag.reshape(rows, LANES, n)])
    s1 = s1.transpose(3, 0, 1, 2).reshape(2 * first_len, LANES)

    vmem = pl.BlockSpec(memory_space=pltpu.VMEM)
    shape = jax.ShapeDtypeStruct((first_len, LANES), jnp.float32)
    work = pltpu.VMEM((2 * first_len, LANES), jnp.float32)
    out_re, out_im = pl.pallas_call(
        functools.partial(kernel, n, rows),
        out_shape=(shape, shape),
        in_specs=[vmem] * 7,
        out_specs=(vmem, vmem),
        scratch_shapes=[
            work,
            work,
            work,
            work,
            work,
            pltpu.SemaphoreType.DMA((n,)),
            pltpu.SemaphoreType.DMA((3, n)),
        ],
        compiler_params=pltpu.CompilerParams(
            has_side_effects=True, vmem_limit_bytes=60 * 1024 * 1024
        ),
    )(s1, t1, t2, tw, t3, tw3, t4)
    return out_re.reshape(local_len), out_im.reshape(local_len)


def solution(mesh):
    in_specs = (P("pa"), P("pa"))
    out_specs = (P("pa"), P("pa"))
    return jax.shard_map(body, mesh=mesh, in_specs=in_specs, out_specs=out_specs, check_vma=False)
```
